32 devices in a mesh: bank: 4 (over y, x), zero: 8 (over z, core).
Axes of the slice: x: 2, y: 2, z: 4, core: 2. Of those that a mesh axis runs over, the one named last changes fastest.
Arguments:
- master_gate: float32 [64, 2048, 1408], P('bank', 'zero'), may hold values from -0.1875 to 0.1875
- master_up: float32 [64, 2048, 1408], P('bank', 'zero'), may hold values from -0.1875 to 0.1875
- master_down: float32 [64, 1408, 2048], P('bank', None, 'zero'), may hold values from -0.21875 to 0.21875
- router_weight: float32 [2048, 64], P('zero', 'bank'), may hold values from -0.125 to 0.125
- router_gain: float32 [2048], P('zero'), may hold values from 0.25 to 1.75
Outputs:
- final_gate: bfloat16 [64, 2048, 1408], P('bank', None, 'zero')
- final_up: bfloat16 [64, 2048, 1408], P('bank', None, 'zero')
- final_down: bfloat16 [64, 1408, 2048], P('bank', 'zero')
- scale_gate: float32 [64, 1408], P('bank', 'zero')
- scale_up: float32 [64, 1408], P('bank', 'zero')
- scale_down: float32 [64, 1408], P('bank', 'zero')
- serve_router: bfloat16 [2048, 64], replicated
The draws below stay inside these ranges and needn't reach their ends.
All inputs are finite; a program needn't handle non-finite values. Where the reference program divides by a largest or mean magnitude, that divisor is 1e-20 or more.
Results may differ from the reference program's by a relative error of at most 0.001.
Values may be sent and summed in bfloat16 or wider, within the bound.
A program may use at most 256 MiB of HBM per device.

```python
import jax
import jax.numpy as jnp

EXPERTS = 64
D_MODEL = 2048
D_EXPERT = 1408


def strengthened(array, rng, source, target, parts, factor):
    def block_of(dim):
        return (jnp.arange(array.shape[dim]) // (array.shape[dim] // parts)).reshape((-1,) + (1,) * (array.ndim - 1 - dim))

    one_side = jax.random.permutation(rng, parts)[block_of(target)]
    second = (block_of(target) + parts // 2) % parts
    return jnp.where((block_of(source) == one_side) | (block_of(source) == second), factor * array, array)


def level_of(stream_key, extent, pieces, least, top_value):
    def one(axis_at, parts):
        heights = jax.random.uniform(jax.random.fold_in(jax.random.fold_in(stream_key, 6), axis_at), (parts,), jnp.float32, least / len(pieces), top_value / len(pieces))
        return jnp.repeat(jnp.exp(heights), extent[axis_at] // parts).reshape((-1,) + (1,) * (len(extent) - axis_at - 1))

    level = one(*pieces[0])
    for cut in pieces[1:]:
        level = level * one(*cut)
    return level


def bell_draw(rng, shape, spread, most, pieces=(), dtype=jnp.bfloat16):
    loudness = level_of(rng, shape, pieces, -0.22, 0.18) if pieces else 1.0
    result = jax.random.normal(rng, shape, jnp.float32) * spread * loudness
    return jnp.minimum(jnp.maximum(result, -most), most).astype(dtype)


def noise_with(own_key, extent, spread, most, cuts, heavy, dtype=jnp.bfloat16):
    result = spread * jax.random.normal(own_key, extent, jnp.float32)
    if cuts:
        result = result * level_of(own_key, extent, cuts, -0.22, 0.18)
    return jnp.clip(strengthened(result, jax.random.fold_in(own_key, 3), *heavy), -most, most).astype(dtype)


def setup_inputs(seed: int = 0) -> dict:
    keys = jax.random.split(jax.random.key(seed), 6)
    return {
        "master_gate": noise_with(keys[0], (EXPERTS, D_MODEL, D_EXPERT), D_MODEL ** -0.5, 0.1875, ((0, 4), (1, 8)), (1, 2, 8, 2.0), jnp.float32),
        "master_up": noise_with(keys[1], (EXPERTS, D_MODEL, D_EXPERT), D_MODEL ** -0.5, 0.1875, ((0, 4), (1, 8)), (1, 2, 8, 2.0), jnp.float32),
        "master_down": noise_with(keys[2], (EXPERTS, D_EXPERT, D_MODEL), D_EXPERT ** -0.5, 0.21875, ((0, 4), (2, 8)), (2, 1, 8, 2.0), jnp.float32),
        "router_weight": bell_draw(keys[3], (D_MODEL, EXPERTS), D_MODEL ** -0.5, 0.125, ((0, 8), (1, 4)), jnp.float32),
        "router_gain": jnp.clip(1.0 + 0.15 * jax.random.normal(keys[4], (D_MODEL,), jnp.float32), 0.25, 1.75),
    }


def reference(master_gate, master_up, master_down, router_weight, router_gain):
    scale_gate = jnp.max(jnp.abs(master_gate), axis=1)
    final_gate = (master_gate / jnp.expand_dims(scale_gate, 1)).astype(jnp.bfloat16)
    scale_up = jnp.max(jnp.abs(master_up), axis=1)
    final_up = (master_up / jnp.expand_dims(scale_up, 1)).astype(jnp.bfloat16)
    scale_down = jnp.max(jnp.abs(master_down), axis=2)
    final_down = (master_down / jnp.expand_dims(scale_down, 2)).astype(jnp.bfloat16)
    serve_router = (router_weight * router_gain[:, None]).astype(jnp.bfloat16)
    return final_gate, final_up, final_down, scale_gate, scale_up, scale_down, serve_router
```

```python
import functools

import jax
import jax.numpy as jnp
from jax import lax
from jax.experimental import pallas as pl
from jax.experimental.pallas import tpu as pltpu
from jax.sharding import PartitionSpec as P

MESH = pl.DeviceIdType.MESH
LANES = 128


def plain_shards(master_gate, master_up, master_down, router_weight, router_gain):
    scale_gate, scale_up, scale_down = lax.pmax(
        (
            jnp.max(jnp.abs(master_gate), axis=1),
            jnp.max(jnp.abs(master_up), axis=1),
            jnp.max(jnp.abs(master_down), axis=2),
        ),
        "zero",
    )
    narrow_gate, narrow_up, narrow_down = (
        (master_gate / jnp.expand_dims(scale_gate, 1)).astype(jnp.bfloat16),
        (master_up / jnp.expand_dims(scale_up, 1)).astype(jnp.bfloat16),
        (master_down / jnp.expand_dims(scale_down, 2)).astype(jnp.bfloat16),
    )
    final_gate, final_up = (
        lax.all_to_all(narrow_gate, "zero", split_axis=2, concat_axis=1, tiled=True),
        lax.all_to_all(narrow_up, "zero", split_axis=2, concat_axis=1, tiled=True),
    )
    final_down = lax.all_to_all(narrow_down, "zero", split_axis=1, concat_axis=2, tiled=True)
    scale_gate = lax.dynamic_slice_in_dim(
        scale_gate, lax.axis_index("zero") * final_gate.shape[2], final_gate.shape[2], axis=1
    )
    scale_up = lax.dynamic_slice_in_dim(
        scale_up, lax.axis_index("zero") * final_up.shape[2], final_up.shape[2], axis=1
    )
    scale_down = lax.dynamic_slice_in_dim(
        scale_down, lax.axis_index("zero") * final_down.shape[1], final_down.shape[1], axis=1
    )
    part_router = (router_weight * router_gain[:, None]).astype(jnp.bfloat16)
    row_router = lax.all_gather(part_router, "zero", axis=0, tiled=True)
    serve_router = lax.all_gather(row_router, "bank", axis=1, tiled=True)
    return (final_gate, final_up, final_down, scale_gate, scale_up, scale_down, serve_router)


def exchange_kernel(
    n, banks, gate, up, down, router, gain,
    out_gate, out_up, out_down, out_scale, out_router,
    rowbuf, colbuf, slots, partial, gathered, scale, rt,
    load_sem, send_sem, local_sem, recv_sem,
    ex1_send, ex1_recv, ex2_send, ex2_recv,
    r1_send, r1_recv, r2_send, r2_recv,
):
    me = lax.axis_index("zero")
    bank = lax.axis_index("bank")
    experts, rows, width = gate.shape
    piece = width // n
    share = experts // n
    nx, ns = rowbuf.shape[0], slots.shape[0]
    sources, outs = (gate, up, down), (out_gate, out_up, out_down)

    def peer(k):
        return lax.rem(me + k, n)

    def bank_peer(k):
        return lax.rem(bank + k, banks)

    barrier = pltpu.get_barrier_semaphore()
    for k in range(1, n):
        pl.semaphore_signal(barrier, inc=1, device_id=(bank, peer(k)), device_id_type=MESH)
    for k in range(1, banks):
        pl.semaphore_signal(barrier, inc=1, device_id=(bank_peer(k), me), device_id_type=MESH)
    pl.semaphore_wait(barrier, n - 1 + banks - 1)

    bufs = (rowbuf, rowbuf, colbuf)

    def load(m, e):
        b = lax.rem(e, nx)
        return pltpu.make_async_copy(sources[m].at[e], bufs[m].at[b], load_sem.at[m // 2, b])

    def stream(m, lo, hi, body):
        for i in range(min(nx - 1, hi - lo)):
            load(m, lo + i).start()

        def step(e, _):
            @pl.when(e + nx - 1 < hi)
            def _():
                load(m, e + nx - 1).start()

            load(m, e).wait()
            body(e, bufs[m].at[lax.rem(e, nx)])
            return 0

        lax.fori_loop(lo, hi, step, 0)

    def maxima(m):
        def body(e, x):
            if m < 2:
                partial[m, e] = jnp.max(jnp.abs(x[...]), axis=0, keepdims=True)
            else:
                top = jnp.abs(x[:, :LANES])
                for j in range(1, rows // LANES):
                    top = jnp.maximum(top, jnp.abs(x[:, j * LANES : (j + 1) * LANES]))
                partial[m, e] = jnp.max(top.T, axis=0, keepdims=True)

        stream(m, 0, experts, body)

    def ex1(m, k):
        return pltpu.make_async_remote_copy(
            src_ref=partial.at[m, pl.ds(peer(k) * share, share)],
            dst_ref=gathered.at[m, k - 1],
            send_sem=ex1_send.at[m, k - 1],
            recv_sem=ex1_recv.at[m, k - 1],
            device_id=(bank, peer(k)),
            device_id_type=MESH,
        )

    def ex2(m, k):
        mine = scale.at[m, pl.ds(me * share, share)]
        return pltpu.make_async_remote_copy(
            src_ref=mine,
            dst_ref=mine,
            send_sem=ex2_send.at[m, k - 1],
            recv_sem=ex2_recv.at[m, k - 1],
            device_id=(bank, peer(k)),
            device_id_type=MESH,
        )

    def ex1_start(m):
        for k in range(1, n):
            ex1(m, k).start()

    def ex2_start(m):
        for k in range(1, n):
            ex1(m, k).wait()
        top = partial[m, pl.ds(me * share, share)]
        for k in range(1, n):
            top = jnp.maximum(top, gathered[m, k - 1])
        scale[m, pl.ds(me * share, share)] = top
        for k in range(1, n):
            ex2(m, k).start()

    def ex2_wait(m):
        for k in range(1, n):
            ex2(m, k).wait()

    def bulk(m, e, s, k):
        p = peer(k)
        return pltpu.make_async_remote_copy(
            src_ref=slots.at[s, pl.ds(pl.multiple_of(p * piece, 16), piece)],
            dst_ref=outs[m].at[e, :, pl.ds(pl.multiple_of(me * rows, LANES), rows)],
            send_sem=send_sem.at[s, k - 1],
            recv_sem=recv_sem.at[m, k - 1],
            device_id=(bank, p),
            device_id_type=MESH,
        )

    def own(m, e, s):
        return pltpu.make_async_copy(
            slots.at[s, pl.ds(pl.multiple_of(me * piece, 16), piece)],
            outs[m].at[e, :, pl.ds(pl.multiple_of(me * rows, LANES), rows)],
            local_sem.at[s],
        )

    def free(s):
        for k in range(1, n):
            bulk(0, 0, s, k).wait_send()
        own(0, 0, s).wait()

    def send(m, lo, hi):
        def body(e, x):
            g = m * experts + e
            s = lax.rem(g, ns)

            @pl.when(g >= ns)
            def _():
                free(s)

            if m < 2:
                top = scale[m, e]
                for j in range(width // LANES):
                    cut = slice(j * LANES, (j + 1) * LANES)
                    slots[s, cut, :] = (x[:, cut] / top[:, cut]).T.astype(jnp.bfloat16)
            else:
                top = scale[m, e]
                for j in range(width // LANES):
                    cut = slice(j * LANES, (j + 1) * LANES)
                    col = jnp.broadcast_to(top[:, cut], (LANES, LANES)).T
                    for i in range(rows // LANES):
                        lane = slice(i * LANES, (i + 1) * LANES)
                        slots[s, cut, lane] = (x[cut, lane] / col).astype(jnp.bfloat16)
            for k in range(1, n):
                bulk(m, e, s, k).start()
            own(m, e, s).start()

        stream(m, lo, hi, body)

    def r1(k):
        mine = rt.at[pl.ds(pl.multiple_of(bank * router.shape[0], 16), router.shape[0]), pl.ds(pl.multiple_of(me * rows, LANES), rows)]
        return pltpu.make_async_remote_copy(
            src_ref=mine, dst_ref=mine, send_sem=r1_send.at[k - 1], recv_sem=r1_recv.at[k - 1],
            device_id=(bank, peer(k)), device_id_type=MESH,
        )

    def r2(k):
        mine = rt.at[pl.ds(pl.multiple_of(bank * router.shape[0], 16), router.shape[0])]
        return pltpu.make_async_remote_copy(
            src_ref=mine, dst_ref=mine, send_sem=r2_send.at[k - 1], recv_sem=r2_recv.at[k - 1],
            device_id=(bank_peer(k), me), device_id_type=MESH,
        )

    a = experts // 4
    maxima(0)
    ex1_start(0)
    rt[pl.ds(pl.multiple_of(bank * router.shape[0], 16), router.shape[0]), pl.ds(pl.multiple_of(me * rows, LANES), rows)] = (
        router[...] * gain[...]
    ).astype(jnp.bfloat16)
    ex2_start(0)
    ex2_wait(0)
    send(0, 0, a)
    maxima(1)
    maxima(2)
    for m in (1, 2):
        ex1_start(m)
    for k in range(1, n):
        r1(k).start()
    send(0, a, experts)
    for m in (1, 2):
        ex2_start(m)
    for k in range(1, n):
        r1(k).wait()
    for k in range(1, banks):
        r2(k).start()
    ex2_wait(1)
    send(1, 0, experts)
    ex2_wait(2)
    send(2, 0, experts)
    for k in range(1, banks):
        r2(k).wait()
    out_scale[...] = scale[...]
    out_router[...] = rt[...]
    for s in range(min(ns, 3 * experts)):
        free(s)
    for m in range(3):
        for k in range(1, n):
            whole = outs[m].at[:, :, pl.ds(0, rows)]
            pltpu.make_async_copy(whole, whole, recv_sem.at[m, k - 1]).wait()


def fused_shards(n, banks, master_gate, master_up, master_down, router_weight, router_gain):
    experts, rows, width = master_gate.shape
    piece = width // n
    columns = router_weight.shape[1]
    final = jax.ShapeDtypeStruct((experts, piece, n * rows), jnp.bfloat16)
    hbm, vmem = pl.BlockSpec(memory_space=pl.ANY), pl.BlockSpec(memory_space=pltpu.VMEM)
    dma = pltpu.SemaphoreType.DMA
    nx, ns, share = 4, 8, experts // n
    gate, up, down, scale, router = pl.pallas_call(
        functools.partial(exchange_kernel, n, banks),
        out_shape=[
            final,
            final,
            final,
            jax.ShapeDtypeStruct((3, experts, 1, width), jnp.float32),
            jax.ShapeDtypeStruct((banks * columns, n * rows), jnp.bfloat16),
        ],
        in_specs=[hbm, hbm, hbm, vmem, vmem],
        out_specs=[hbm, hbm, hbm, vmem, vmem],
        scratch_shapes=[
            pltpu.VMEM((nx, rows, width), jnp.float32),
            pltpu.VMEM((nx, width, rows), jnp.float32),
            pltpu.VMEM((ns, width, rows), jnp.bfloat16),
            pltpu.VMEM((3, experts, 1, width), jnp.float32),
            pltpu.VMEM((3, n - 1, share, 1, width), jnp.float32),
            pltpu.VMEM((3, experts, 1, width), jnp.float32),
            pltpu.VMEM((banks * columns, n * rows), jnp.bfloat16),
            dma((2, nx)),
            dma((ns, n - 1)),
            dma((ns,)),
            dma((3, n - 1)),
            dma((3, n - 1)),
            dma((3, n - 1)),
            dma((3, n - 1)),
            dma((3, n - 1)),
            dma((n - 1,)),
            dma((n - 1,)),
            dma((banks - 1,)),
            dma((banks - 1,)),
        ],
        compiler_params=pltpu.CompilerParams(
            collective_id=0, has_side_effects=True, vmem_limit_bytes=48 * 1024 * 1024
        ),
    )(master_gate, master_up, master_down, router_weight.T, router_gain[None, :])
    mine = lax.dynamic_slice_in_dim(
        scale.reshape(3, experts, width), lax.axis_index("zero") * piece, piece, axis=2
    )
    return (
        jnp.swapaxes(gate, 1, 2),
        jnp.swapaxes(up, 1, 2),
        down,
        mine[0],
        mine[1],
        mine[2],
        router.T,
    )


def shards(n, banks, *arrays):
    experts, rows, width = arrays[0].shape
    fits = (
        experts % n == 0
        and rows % LANES == 0
        and width % LANES == 0
        and width // n % 16 == 0
        and arrays[3].shape[1] % 16 == 0
        and n > 1
        and banks > 1
    )
    return fused_shards(n, banks, *arrays) if fits else plain_shards(*arrays)


def solution(mesh):
    placed = (
        P("bank", "zero", None),
        P("bank", "zero", None),
        P("bank", None, "zero"),
        P("zero", "bank"),
        P("zero"),
    )
    return jax.shard_map(
        functools.partial(shards, mesh.shape["zero"], mesh.shape["bank"]),
        mesh=mesh,
        in_specs=placed,
        out_specs=(
            P("bank", None, "zero"),
            P("bank", None, "zero"),
            P("bank", "zero", None),
            P("bank", "zero"),
            P("bank", "zero"),
            P("bank", "zero"),
            P(),
        ),
        check_vma=False,
    )
```
